32 devices in a mesh: dp: 2 (over x), tp: 4 (over z), cp: 4 (over y, core).
Axes of the slice: x: 2, y: 2, z: 4, core: 2. Of those that a mesh axis runs over, the one named last changes fastest.
Arguments:
- hidden: bfloat16 [4096, 5120], P(('dp', 'cp', 'tp')), parts along dimension 0
- positions: int32 [4096], P(('dp', 'cp', 'tp')), parts along dimension 0
- doc_ids: int32 [4096], P(('dp', 'cp', 'tp')), parts along dimension 0
- attn_gain: bfloat16 [5120], replicated
- mlp_gain: bfloat16 [5120], replicated
- w_query: bfloat16 [5120, 5120], P(None, 'tp')
- w_key: bfloat16 [5120, 1024], P(None, 'tp')
- w_value: bfloat16 [5120, 1024], P(None, 'tp')
- w_out: bfloat16 [5120, 5120], P('tp')
- w_gate: bfloat16 [5120, 27648], P(None, 'tp')
- w_up: bfloat16 [5120, 27648], P(None, 'tp')
- w_down: bfloat16 [27648, 5120], P('tp')
Outputs:
- output: bfloat16 [4096, 5120], P(('dp', 'cp', 'tp')), parts along dimension 0
There are 2 independent parts. The reference program is written for one: setup_inputs(seed, part) draws one part's arguments, and reference() takes and returns one part's arrays. A program takes and returns all parts, laid end to end along the dimension named above; an argument that names none is the same for every part.
All inputs are finite; a program needn't handle non-finite values.
Results may differ from the reference program's by a relative error of at most 0.0125486.
Values are sent between devices in bfloat16 or wider.
A program may use at most 1 GiB of HBM per device.

```python
import math
import jax
import jax.numpy as jnp
from jax import lax

ROWS_DEV = 128
SHARDS = 16
MODEL_DIM = 5120
Q_HEADS = 40
KV_HEADS = 8
HEAD_DIM = 128
FFN_DIM = 27648
NUM_DOCS = 4
TOKENS = ROWS_DEV * SHARDS
Q_BLOCK = math.gcd(TOKENS, 32)
SCORE_VAR = math.log(TOKENS / 16.0)
ROPE_BASE = 500000.0
NORM_EPS = 1e-5
NEG_BIG = -1e30


def arrange(values):
    pieces = values.reshape(2 * SHARDS, TOKENS // (2 * SHARDS))
    return jnp.stack([pieces[:SHARDS], pieces[SHARDS:][::-1]], axis=1).reshape(TOKENS)


def doc_layout(doc_key):
    cut_points = jnp.sort(jax.random.permutation(doc_key, TOKENS - 1)[: NUM_DOCS - 1] + 1).astype(jnp.int32)
    logical = jnp.arange(TOKENS, dtype=jnp.int32)
    doc_logical = jnp.sum((logical[:, None] >= cut_points[None, :]).astype(jnp.int32), axis=1)
    starts = jnp.concatenate([jnp.zeros((1,), jnp.int32), cut_points])
    pos_logical = logical - starts[doc_logical]
    return arrange(pos_logical), arrange(doc_logical)


def normal_weight(weight_key, arr_shape, std_scale):
    return (jax.random.normal(weight_key, arr_shape, jnp.float32) * std_scale).astype(jnp.bfloat16)


def setup_inputs(seed: int = 0, part: int = 0) -> dict:
    base_key = jax.random.key(seed)
    part_key = jax.random.fold_in(base_key, part)
    hidden_key, doc_key = jax.random.split(part_key)
    weight_keys = jax.random.split(base_key, 9)
    positions, doc_ids = doc_layout(doc_key)
    q_cols = Q_HEADS * HEAD_DIM
    kv_cols = KV_HEADS * HEAD_DIM
    qk_scale = SCORE_VAR ** 0.25 * MODEL_DIM ** -0.5
    return {
        'hidden': normal_weight(hidden_key, (TOKENS, MODEL_DIM), 1.0),
        'positions': positions,
        'doc_ids': doc_ids,
        'attn_gain': (1.0 + 0.25 * jax.random.normal(weight_keys[0], (MODEL_DIM,), jnp.float32)).astype(jnp.bfloat16),
        'mlp_gain': (1.0 + 0.25 * jax.random.normal(weight_keys[1], (MODEL_DIM,), jnp.float32)).astype(jnp.bfloat16),
        'w_query': normal_weight(weight_keys[2], (MODEL_DIM, q_cols), qk_scale),
        'w_key': normal_weight(weight_keys[3], (MODEL_DIM, kv_cols), qk_scale),
        'w_value': normal_weight(weight_keys[4], (MODEL_DIM, kv_cols), MODEL_DIM ** -0.5),
        'w_out': normal_weight(weight_keys[5], (q_cols, MODEL_DIM), q_cols ** -0.5),
        'w_gate': normal_weight(weight_keys[6], (MODEL_DIM, FFN_DIM), MODEL_DIM ** -0.5),
        'w_up': normal_weight(weight_keys[7], (MODEL_DIM, FFN_DIM), MODEL_DIM ** -0.5),
        'w_down': normal_weight(weight_keys[8], (FFN_DIM, MODEL_DIM), FFN_DIM ** -0.5),
    }


def rms_norm(values, gain_vec):
    wide_vals = values.astype(jnp.float32)
    inv_rms = lax.rsqrt(jnp.mean(wide_vals * wide_vals, axis=-1, keepdims=True) + NORM_EPS)
    return (wide_vals * inv_rms * gain_vec.astype(jnp.float32)).astype(jnp.bfloat16)


def rotary(vectors, positions):
    half_dim = vectors.shape[-1] // 2
    inv_freq = ROPE_BASE ** (-jnp.arange(half_dim, dtype=jnp.float32) * (2.0 / vectors.shape[-1]))
    angles = positions.astype(jnp.float32)[:, None] * inv_freq[None, :]
    cos_ang = jnp.cos(angles)[:, None, :]
    sin_ang = jnp.sin(angles)[:, None, :]
    first_half = vectors[..., :half_dim]
    second_half = vectors[..., half_dim:]
    return jnp.concatenate([first_half * cos_ang - second_half * sin_ang, second_half * cos_ang + first_half * sin_ang], axis=-1)


def reference(hidden, positions, doc_ids, attn_gain, mlp_gain, w_query, w_key, w_value, w_out, w_gate, w_up, w_down):
    group_size = Q_HEADS // KV_HEADS
    normed = rms_norm(hidden, attn_gain)
    queries = rotary(jnp.dot(normed, w_query, preferred_element_type=jnp.float32).reshape(TOKENS, Q_HEADS, HEAD_DIM), positions).astype(jnp.bfloat16)
    keys_rot = rotary(jnp.dot(normed, w_key, preferred_element_type=jnp.float32).reshape(TOKENS, KV_HEADS, HEAD_DIM), positions).astype(jnp.bfloat16)
    values_all = jnp.dot(normed, w_value, preferred_element_type=jnp.float32).astype(jnp.bfloat16).reshape(TOKENS, KV_HEADS, HEAD_DIM)
    keys_wide = keys_rot.astype(jnp.float32)
    values_wide = values_all.astype(jnp.float32)
    n_blocks = TOKENS // Q_BLOCK
    q_blocks = queries.reshape(n_blocks, Q_BLOCK, KV_HEADS, group_size, HEAD_DIM)
    pos_blocks = positions.reshape(n_blocks, Q_BLOCK)
    doc_blocks = doc_ids.reshape(n_blocks, Q_BLOCK)

    def attend(block_in):
        q_blk, query_pos, query_doc = block_in
        scores = jnp.einsum('qhgd,khd->hgqk', q_blk.astype(jnp.float32), keys_wide) * (HEAD_DIM ** -0.5)
        visible = (query_doc[:, None] == doc_ids[None, :]) & (positions[None, :] <= query_pos[:, None])
        scores = jnp.where(visible, scores, NEG_BIG)
        row_max = jnp.max(scores, axis=-1, keepdims=True)
        weights = jnp.where(visible, jnp.exp(scores - row_max), 0.0)
        row_sum = jnp.sum(weights, axis=-1, keepdims=True)
        block_mix = jnp.einsum('hgqk,khd->hgqd', weights.astype(jnp.bfloat16).astype(jnp.float32), values_wide) / row_sum
        return jnp.transpose(block_mix, (2, 0, 1, 3)).astype(jnp.bfloat16)

    attn_mix = lax.map(attend, (q_blocks, pos_blocks, doc_blocks)).reshape(TOKENS, Q_HEADS * HEAD_DIM)
    attn_out = jnp.dot(attn_mix, w_out, preferred_element_type=jnp.float32)
    residual = (hidden.astype(jnp.float32) + attn_out).astype(jnp.bfloat16)
    normed_mlp = rms_norm(residual, mlp_gain)
    gate_val = jnp.dot(normed_mlp, w_gate, preferred_element_type=jnp.float32)
    up_val = jnp.dot(normed_mlp, w_up, preferred_element_type=jnp.float32)
    gated = (jax.nn.silu(gate_val) * up_val).astype(jnp.bfloat16)
    down_val = jnp.dot(gated, w_down, preferred_element_type=jnp.float32)
    return (residual.astype(jnp.float32) + down_val).astype(jnp.bfloat16)
```

```python
import functools

import jax
import jax.numpy as jnp
from jax import lax
from jax.experimental import pallas as pl
from jax.experimental.pallas import tpu as pltpu
from jax.sharding import PartitionSpec as P

HEAD_DIM = 128
ROPE_BASE = 500000.0
NORM_EPS = 1e-5
NEG_BIG = -1e30
MESH = pl.DeviceIdType.MESH
BF16 = jnp.bfloat16
F32 = jnp.float32
VMEM_LIMIT = 67043328

TP = 4
ROWS = 128
DIM = 5120
KC = 512
NK = DIM // KC
CC = 256
NCC = DIM // CC
PER = KC // CC
FILL = 4


def tp_barrier(z):
    barrier = pltpu.get_barrier_semaphore()
    for peer in range(TP):
        @pl.when(z != peer)
        def _():
            pl.semaphore_signal(barrier, inc=1, device_id={"tp": peer}, device_id_type=MESH)
    pl.semaphore_wait(barrier, TP - 1)


def gather_tools(z, bg, r_right, r_left, s_right, s_left):
    def blk(origin, chunk):
        lane = pl.multiple_of((chunk % PER) * CC, CC)
        return bg.at[chunk // PER, pl.ds(pl.multiple_of(origin * ROWS, ROWS), ROWS), pl.ds(lane, CC)]

    def right(dist, chunk):
        ref = blk(z - dist, chunk)
        return pltpu.make_async_remote_copy(ref, ref, s_right.at[dist, chunk], r_right.at[dist, chunk],
                                            device_id={"tp": jnp.minimum(z + 1, TP - 1)}, device_id_type=MESH)

    def left(dist, chunk):
        ref = blk(z + dist, chunk)
        return pltpu.make_async_remote_copy(ref, ref, s_left.at[dist, chunk], r_left.at[dist, chunk],
                                            device_id={"tp": jnp.maximum(z - 1, 0)}, device_id_type=MESH)

    def got_right(dist, chunk):
        ref = blk(z - 1 - dist, chunk)
        return pltpu.make_async_remote_copy(ref, ref, s_right.at[dist, chunk], r_right.at[dist, chunk],
                                            device_id={"tp": jnp.maximum(z - 1, 0)}, device_id_type=MESH)

    def got_left(dist, chunk):
        ref = blk(z + 1 + dist, chunk)
        return pltpu.make_async_remote_copy(ref, ref, s_left.at[dist, chunk], r_left.at[dist, chunk],
                                            device_id={"tp": jnp.minimum(z + 1, TP - 1)}, device_id_type=MESH)

    def tick(t):
        @pl.when((z < TP - 1) & (t < NCC))
        def _():
            right(0, t).start()

        @pl.when((z > 0) & (t < NCC))
        def _():
            left(0, t).start()

        for d in (1, 2):
            c = t - d
            ok = (c >= 0) & (c < NCC)

            @pl.when(ok & (z < TP - 1) & (z >= d))
            def _():
                got_right(d - 1, c).wait_recv()
                right(d, c).start()

            @pl.when(ok & (z > 0) & (z + d <= TP - 1))
            def _():
                got_left(d - 1, c).wait_recv()
                left(d, c).start()

    def arrived(g):
        @pl.when(z == TP - 1)
        def _():
            for d in range(TP - 1):
                for k in range(PER):
                    got_right(d, g * PER + k).wait_recv()

        @pl.when(z == 0)
        def _():
            for d in range(TP - 1):
                for k in range(PER):
                    got_left(d, g * PER + k).wait_recv()

    def drain():
        def body(c, _):
            for d in range(TP - 1):
                @pl.when((z < TP - 1) & (z >= d))
                def _():
                    right(d, c).wait_send()

                @pl.when((z > 0) & (z + d <= TP - 1))
                def _():
                    left(d, c).wait_send()
            return 0
        lax.fori_loop(0, NCC, body, 0)

    return tick, arrived, drain


def norm_into(z, x_ref, gain_ref, bg):
    def body(i, _):
        r0 = pl.multiple_of(i * 16, 16)
        wide = x_ref[pl.ds(r0, 16), :].astype(F32)
        inv = lax.rsqrt(jnp.mean(wide * wide, axis=-1, keepdims=True) + NORM_EPS)
        out = (wide * inv * gain_ref[...].astype(F32)).astype(BF16)
        row = pl.multiple_of(z * ROWS + r0, 16)
        for g in range(NK):
            bg[g, pl.ds(row, 16), :] = out[:, g * KC:(g + 1) * KC]
        return 0
    lax.fori_loop(0, ROWS // 16, body, 0)


GATHER_SEMS = [pltpu.SemaphoreType.DMA((TP - 1, NCC))] * 4

QT = 2304
SLOTS = 4


def gate_up_kernel(n_tiles, x_ref, gain_ref, wg, wu, out_ref, bg, acc, wbuf, wsem, r_right, r_left, s_right, s_left):
    z = lax.axis_index("tp")
    total = NK * 2 * n_tiles

    def fetch(i, start):
        q = i % (2 * n_tiles)
        k0 = pl.multiple_of((i // (2 * n_tiles)) * KC, KC)
        n0 = pl.multiple_of((q % n_tiles) * QT, QT)
        slot = i % SLOTS

        @pl.when(q < n_tiles)
        def _():
            c = pltpu.make_async_copy(wg.at[pl.ds(k0, KC), pl.ds(n0, QT)], wbuf.at[slot], wsem.at[slot])
            c.start() if start else c.wait()

        @pl.when(q >= n_tiles)
        def _():
            c = pltpu.make_async_copy(wu.at[pl.ds(k0, KC), pl.ds(n0, QT)], wbuf.at[slot], wsem.at[slot])
            c.start() if start else c.wait()

    for i in range(SLOTS - 1):
        fetch(i, True)
    norm_into(z, x_ref, gain_ref, bg)
    tp_barrier(z)
    tick, arrived, drain = gather_tools(z, bg, r_right, r_left, s_right, s_left)
    tick(0)

    def zero(i, _):
        q = i // 16
        r0 = pl.multiple_of((i % 16) * 32, 32)
        acc[q, pl.ds(r0, 32), :] = jnp.zeros((32, QT), F32)
        return 0
    lax.fori_loop(0, 2 * n_tiles * 16, zero, 0)
    for t in range(1, FILL):
        tick(t)

    def step(u, _):
        tick(u + FILL)
        g = u // 2

        @pl.when(u % 2 == 0)
        def _():
            arrived(g)

        def tile(j, _):
            i = u * n_tiles + j
            fetch(i, False)

            @pl.when(i + SLOTS - 1 < total)
            def _():
                fetch(i + SLOTS - 1, True)
            q = i % (2 * n_tiles)
            acc[q] += jnp.dot(bg[g], wbuf[i % SLOTS], preferred_element_type=F32)
            return 0
        lax.fori_loop(0, n_tiles, tile, 0)
        return 0
    lax.fori_loop(0, 2 * NK, step, 0)

    def finish(i, _):
        r0 = pl.multiple_of(i * 16, 16)
        for j in range(n_tiles):
            gate = acc[j, pl.ds(r0, 16), :]
            up = acc[n_tiles + j, pl.ds(r0, 16), :]
            out_ref[pl.ds(r0, 16), j * QT:(j + 1) * QT] = (jax.nn.silu(gate) * up).astype(BF16)
        return 0
    lax.fori_loop(0, TP * ROWS // 16, finish, 0)
    drain()


def gate_up(x, gain, wg, wu):
    ffn = wg.shape[1]
    n_tiles = ffn // QT
    vm = pl.BlockSpec(memory_space=pltpu.VMEM)
    hbm = pl.BlockSpec(memory_space=pl.ANY)
    return pl.pallas_call(
        functools.partial(gate_up_kernel, n_tiles),
        out_shape=jax.ShapeDtypeStruct((TP * ROWS, ffn), BF16),
        in_specs=[vm, vm, hbm, hbm],
        out_specs=vm,
        scratch_shapes=[
            pltpu.VMEM((NK, TP * ROWS, KC), BF16),
            pltpu.VMEM((2 * n_tiles, TP * ROWS, QT), F32),
            pltpu.VMEM((SLOTS, KC, QT), BF16),
            pltpu.SemaphoreType.DMA((SLOTS,)),
        ] + GATHER_SEMS,
        compiler_params=pltpu.CompilerParams(collective_id=2, has_side_effects=True, vmem_limit_bytes=VMEM_LIMIT),
        name="gate_up",
    )(x, gain.reshape(1, -1), wg, wu)


def qkv_kernel(x_ref, gain_ref, pos_ref, wq, wk, wv, out_ref, pos_out, bg, wbuf, wsem, psend, precv, r_right, r_left, s_right, s_left):
    z = lax.axis_index("tp")
    nq, nkv = wq.shape[1], wk.shape[1]

    def fetch(g, start):
        k0 = pl.multiple_of(g * KC, KC)
        slot = g % 2
        for idx, (w, off, width) in enumerate(((wq, 0, nq), (wk, nq, nkv), (wv, nq + nkv, nkv))):
            c = pltpu.make_async_copy(w.at[pl.ds(k0, KC), :], wbuf.at[slot, :, pl.ds(off, width)], wsem.at[slot, idx])
            c.start() if start else c.wait()

    fetch(0, True)
    fetch(1, True)
    pos_out[z] = pos_ref[...]
    norm_into(z, x_ref, gain_ref, bg)
    tp_barrier(z)
    tick, arrived, drain = gather_tools(z, bg, r_right, r_left, s_right, s_left)

    def pos_copy(peer, origin):
        return pltpu.make_async_remote_copy(pos_ref, pos_out.at[origin], psend.at[peer], precv.at[origin],
                                            device_id={"tp": peer}, device_id_type=MESH)
    tick(0)
    for peer in range(TP):
        @pl.when(z != peer)
        def _():
            pos_copy(peer, z).start()
    out_ref[...] = jnp.zeros(out_ref.shape, F32)
    for t in range(1, FILL):
        tick(t)

    def step(g, _):
        for h in range(2):
            tick(g * 2 + h + FILL)
        arrived(g)
        fetch(g, False)
        out_ref[...] += jnp.dot(bg[g], wbuf[g % 2], preferred_element_type=F32)

        @pl.when(g + 2 < NK)
        def _():
            fetch(g + 2, True)
        return 0
    lax.fori_loop(0, NK, step, 0)
    for peer in range(TP):
        @pl.when(z != peer)
        def _():
            pos_copy(peer, z).wait_send()
            pos_copy(peer, peer).wait_recv()
    drain()


def qkv_proj(x, gain, pos, wq, wk, wv):
    width = wq.shape[1] + wk.shape[1] + wv.shape[1]
    vm = pl.BlockSpec(memory_space=pltpu.VMEM)
    hbm = pl.BlockSpec(memory_space=pl.ANY)
    return pl.pallas_call(
        qkv_kernel,
        out_shape=(jax.ShapeDtypeStruct((TP * ROWS, width), F32), jax.ShapeDtypeStruct((TP, 8, ROWS), jnp.int32)),
        in_specs=[vm, vm, vm, hbm, hbm, hbm],
        out_specs=(vm, vm),
        scratch_shapes=[
            pltpu.VMEM((NK, TP * ROWS, KC), BF16),
            pltpu.VMEM((2, KC, width), BF16),
            pltpu.SemaphoreType.DMA((2, 3)),
            pltpu.SemaphoreType.DMA((TP,)),
            pltpu.SemaphoreType.DMA((TP,)),
        ] + GATHER_SEMS,
        compiler_params=pltpu.CompilerParams(collective_id=1, has_side_effects=True, vmem_limit_bytes=VMEM_LIMIT),
        name="qkv_proj",
    )(x, gain.reshape(1, -1), jnp.broadcast_to(pos[None, :], (8, ROWS)), wq, wk, wv)


NC = 512
NN = DIM // NC


def scatter_kernel(lhs, w, res_ref, out_ref, part, from_left, from_right, wbuf, wsem, r_right, r_left, ssem):
    z = lax.axis_index("tp")

    def fetch(c):
        return pltpu.make_async_copy(w.at[:, pl.ds(pl.multiple_of(c * NC, NC), NC)], wbuf.at[c % 2], wsem.at[c % 2])

    fetch(0).start()
    fetch(1).start()
    tp_barrier(z)

    def send_right(c, dest):
        return pltpu.make_async_remote_copy(part.at[c, dest], from_left.at[c, dest - 1], ssem.at[c, dest], r_right.at[c, dest - 1],
                                            device_id={"tp": jnp.minimum(z + 1, TP - 1)}, device_id_type=MESH)

    def send_left(c, dest):
        return pltpu.make_async_remote_copy(part.at[c, dest], from_right.at[c, dest], ssem.at[c, dest], r_left.at[c, dest],
                                            device_id={"tp": jnp.maximum(z - 1, 0)}, device_id_type=MESH)

    def got_left(c, dest):
        return pltpu.make_async_remote_copy(part.at[c, dest], from_left.at[c, dest - 1], ssem.at[c, dest], r_right.at[c, dest - 1],
                                            device_id={"tp": jnp.maximum(z - 1, 0)}, device_id_type=MESH)

    def got_right(c, dest):
        return pltpu.make_async_remote_copy(part.at[c, dest], from_right.at[c, dest], ssem.at[c, dest], r_left.at[c, dest],
                                            device_id={"tp": jnp.minimum(z + 1, TP - 1)}, device_id_type=MESH)

    def step(t, _):
        @pl.when(t < NN)
        def _():
            fetch(t).wait()
            for half in range(2):
                cols = slice(half * NC // 2, (half + 1) * NC // 2)
                prod = jnp.dot(lhs[...], wbuf[t % 2, :, cols], preferred_element_type=F32).astype(BF16)
                for dest in range(TP):
                    part[t, dest, :, cols] = prod[dest * ROWS:(dest + 1) * ROWS]

            @pl.when(t + 2 < NN)
            def _():
                fetch(t + 2).start()

        cr = t - z
        ok_r = (cr >= 0) & (cr < NN)
        cl = t - (TP - 1 - z)
        ok_l = (cl >= 0) & (cl < NN)
        for k in range(TP - 1):
            dest = TP - 1 - k

            @pl.when(ok_r & (dest > z))
            def _():
                @pl.when(z > 0)
                def _():
                    got_left(cr, dest).wait_recv()
                    part[cr, dest] = (part[cr, dest].astype(F32) + from_left[cr, dest - 1].astype(F32)).astype(BF16)
                send_right(cr, dest).start()

            dst = k

            @pl.when(ok_l & (dst < z))
            def _():
                @pl.when(z < TP - 1)
                def _():
                    got_right(cl, dst).wait_recv()
                    part[cl, dst] = (part[cl, dst].astype(F32) + from_right[cl, dst].astype(F32)).astype(BF16)
                send_left(cl, dst).start()

        cf = t - (TP - 1)

        @pl.when(cf >= 0)
        def _():
            cols = pl.ds(pl.multiple_of(jnp.maximum(cf, 0) * NC, NC), NC)

            @pl.when(z > 0)
            def _():
                got_left(cf, z).wait_recv()
                part[cf, z] = (part[cf, z].astype(F32) + from_left[cf, z - 1].astype(F32)).astype(BF16)

            @pl.when(z < TP - 1)
            def _():
                got_right(cf, z).wait_recv()
                part[cf, z] = (part[cf, z].astype(F32) + from_right[cf, z].astype(F32)).astype(BF16)
            out_ref[:, cols] = (res_ref[:, cols].astype(F32) + part[cf, z].astype(F32)).astype(BF16)
        return 0
    lax.fori_loop(0, NN + TP - 1, step, 0)

    def drain(c, _):
        for dest in range(TP):
            @pl.when(dest > z)
            def _():
                send_right(c, max(dest, 1)).wait_send()

            @pl.when(dest < z)
            def _():
                send_left(c, min(dest, TP - 2)).wait_send()
        return 0
    lax.fori_loop(0, NN, drain, 0)


def scatter_proj(lhs, w, res, cid, name):
    depth = w.shape[0]
    vm = pl.BlockSpec(memory_space=pltpu.VMEM)
    hbm = pl.BlockSpec(memory_space=pl.ANY)
    return pl.pallas_call(
        scatter_kernel,
        out_shape=jax.ShapeDtypeStruct((ROWS, DIM), BF16),
        in_specs=[vm, hbm, vm],
        out_specs=vm,
        scratch_shapes=[
            pltpu.VMEM((NN, TP, ROWS, NC), BF16),
            pltpu.VMEM((NN, TP - 1, ROWS, NC), BF16),
            pltpu.VMEM((NN, TP - 1, ROWS, NC), BF16),
            pltpu.VMEM((2, depth, NC), BF16),
            pltpu.SemaphoreType.DMA((2,)),
            pltpu.SemaphoreType.DMA((NN, TP - 1)),
            pltpu.SemaphoreType.DMA((NN, TP - 1)),
            pltpu.SemaphoreType.DMA((NN, TP)),
        ],
        compiler_params=pltpu.CompilerParams(collective_id=cid, has_side_effects=True, vmem_limit_bytes=VMEM_LIMIT),
        name=name,
    )(lhs, w, res)


def rotary(vectors, positions):
    half_dim = vectors.shape[-1] // 2
    inv_freq = ROPE_BASE ** (-jnp.arange(half_dim, dtype=jnp.float32) * (2.0 / vectors.shape[-1]))
    angles = positions.astype(jnp.float32)[:, None] * inv_freq[None, :]
    cos_ang = jnp.cos(angles)[:, None, :]
    sin_ang = jnp.sin(angles)[:, None, :]
    first_half = vectors[..., :half_dim]
    second_half = vectors[..., half_dim:]
    return jnp.concatenate([first_half * cos_ang - second_half * sin_ang, second_half * cos_ang + first_half * sin_ang], axis=-1)


def block_attend(queries, key_blk, val_blk, query_pos, query_doc, key_pos, key_doc, softmax_state):
    row_max, row_sum, accum = softmax_state
    scores = jnp.einsum('qhgd,khd->hgqk', queries, key_blk, preferred_element_type=jnp.float32) * (HEAD_DIM ** -0.5)
    visible = (query_doc[:, None] <= key_doc[None, :]) & (key_doc[None, :] <= query_pos[:, None])
    scores = jnp.where(visible, scores, NEG_BIG)
    new_max = jnp.maximum(row_max, jnp.max(scores, axis=-1))
    weights = jnp.where(visible, jnp.exp(scores - new_max[..., None]), 0.0)
    factor = jnp.exp(row_max - new_max)
    row_sum = row_sum * factor + jnp.sum(weights, axis=-1)
    accum = accum * factor[..., None] + jnp.einsum('hgqk,khd->hgqd', weights.astype(jnp.bfloat16), val_blk, preferred_element_type=jnp.float32)
    return new_max, row_sum, accum


def solution(mesh):
    cp_size = mesh.shape['cp']
    ring_perm = [(idx, (idx + 1) % cp_size) for idx in range(cp_size)]
    row_mat = P(('dp', 'cp', 'tp'), None)
    row_vec = P(('dp', 'cp', 'tp'))
    col_split = P(None, 'tp')
    row_split = P('tp', None)
    pieces = 2 * cp_size * TP
    piece_rows = ROWS // 2

    def logical_rows(cp_idx):
        row = jnp.arange(TP * ROWS, dtype=jnp.int32)
        t, r = row // ROWS, row % ROWS
        k = cp_idx * TP + t
        piece = jnp.where(r < piece_rows, k, pieces - 1 - k)
        return piece * piece_rows + r % piece_rows

    def local_layer(hidden, positions, doc_ids, attn_gain, mlp_gain, w_query, w_key, w_value, w_out, w_gate, w_up, w_down):
        q_local = w_query.shape[1] // HEAD_DIM
        kv_local = w_key.shape[1] // HEAD_DIM
        group_size = q_local // kv_local
        qkv, pos_blk = qkv_proj(hidden, attn_gain, positions, w_query, w_key, w_value)
        pos_all = pos_blk[:, 0, :].reshape(-1)
        row_count = TP * ROWS
        nq, nkv = w_query.shape[1], w_key.shape[1]
        queries = rotary(qkv[:, :nq].reshape(row_count, q_local, HEAD_DIM), pos_all).astype(BF16).reshape(row_count, kv_local, group_size, HEAD_DIM)
        key_own = rotary(qkv[:, nq:nq + nkv].reshape(row_count, kv_local, HEAD_DIM), pos_all).astype(BF16)
        value_own = qkv[:, nq + nkv:].astype(BF16).reshape(row_count, kv_local, HEAD_DIM)
        cp_idx = lax.axis_index('cp')
        q_log = logical_rows(cp_idx)
        q_first = q_log - pos_all
        state = (jnp.full((kv_local, group_size, row_count), NEG_BIG, F32), jnp.zeros((kv_local, group_size, row_count), F32), jnp.zeros((kv_local, group_size, row_count, HEAD_DIM), F32))
        key_blk, val_blk = key_own, value_own
        for s in range(cp_size):
            src = lax.rem(cp_idx - s + cp_size, cp_size)
            state = block_attend(queries, key_blk, val_blk, q_log, q_first, None, logical_rows(src), state)
            if s + 1 < cp_size:
                key_blk = lax.ppermute(key_blk, 'cp', ring_perm)
                val_blk = lax.ppermute(val_blk, 'cp', ring_perm)
        row_max, row_sum, accum = state
        attn_mix = (accum / row_sum[..., None]).astype(BF16)
        attn_mix = attn_mix.transpose(2, 0, 1, 3).reshape(row_count, nq)
        residual = scatter_proj(attn_mix, w_out, hidden, 3, "out_proj")
        gated = gate_up(residual, mlp_gain, w_gate, w_up)
        return scatter_proj(gated, w_down, residual, 4, "down_proj")

    in_specs = (row_mat, row_vec, row_vec, P(None), P(None), col_split, col_split, col_split, row_split, col_split, col_split, row_split)
    return jax.shard_map(local_layer, mesh=mesh, in_specs=in_specs, out_specs=row_mat, check_vma=False)
```

```python
import functools

import jax
import jax.numpy as jnp
from jax import lax
from jax.experimental import pallas as pl
from jax.experimental.pallas import tpu as pltpu
from jax.sharding import PartitionSpec as P

HEAD_DIM = 128
ROPE_BASE = 500000.0
NORM_EPS = 1e-5
NEG_BIG = -1e30
MESH = pl.DeviceIdType.MESH
BF16 = jnp.bfloat16
F32 = jnp.float32
VMEM_LIMIT = 67043328

TP = 4
ROWS = 128
DIM = 5120
KC = 512
NK = DIM // KC
CC = 256
NCC = DIM // CC
PER = KC // CC
HOP = 2
FILL = 2 * HOP + PER
PIECE = ROWS // 2


def tp_signal(z):
    barrier = pltpu.get_barrier_semaphore()
    for peer in range(TP):
        @pl.when(z != peer)
        def _():
            pl.semaphore_signal(barrier, inc=1, device_id={"tp": peer}, device_id_type=MESH)


def tp_wait():
    pl.semaphore_wait(pltpu.get_barrier_semaphore(), TP - 1)


def gather_tools(z, hop, bg, r_right, r_left, s_right, s_left):
    def blk(origin, chunk):
        lane = pl.multiple_of((chunk % PER) * CC, CC)
        return bg.at[chunk // PER, pl.ds(pl.multiple_of(origin * ROWS, ROWS), ROWS), pl.ds(lane, CC)]

    def right(dist, chunk):
        ref = blk(z - dist, chunk)
        return pltpu.make_async_remote_copy(ref, ref, s_right.at[dist, chunk], r_right.at[dist, chunk],
                                            device_id={"tp": jnp.minimum(z + 1, TP - 1)}, device_id_type=MESH)

    def left(dist, chunk):
        ref = blk(z + dist, chunk)
        return pltpu.make_async_remote_copy(ref, ref, s_left.at[dist, chunk], r_left.at[dist, chunk],
                                            device_id={"tp": jnp.maximum(z - 1, 0)}, device_id_type=MESH)

    def got_right(dist, chunk):
        ref = blk(z - 1 - dist, chunk)
        return pltpu.make_async_remote_copy(ref, ref, s_right.at[dist, chunk], r_right.at[dist, chunk],
                                            device_id={"tp": jnp.maximum(z - 1, 0)}, device_id_type=MESH)

    def got_left(dist, chunk):
        ref = blk(z + 1 + dist, chunk)
        return pltpu.make_async_remote_copy(ref, ref, s_left.at[dist, chunk], r_left.at[dist, chunk],
                                            device_id={"tp": jnp.minimum(z + 1, TP - 1)}, device_id_type=MESH)

    def tick(t):
        own = (t >= 0) & (t < NCC)

        @pl.when(own & (z < TP - 1))
        def _():
            right(0, t).start()

        @pl.when(own & (z > 0))
        def _():
            left(0, t).start()

        for d in (1, 2):
            c = t - d * hop
            ok = (c >= 0) & (c < NCC)

            @pl.when(ok & (z < TP - 1) & (z >= d))
            def _():
                got_right(d - 1, c).wait_recv()
                right(d, c).start()

            @pl.when(ok & (z > 0) & (z + d <= TP - 1))
            def _():
                got_left(d - 1, c).wait_recv()
                left(d, c).start()

    def arrived(g):
        @pl.when(z == TP - 1)
        def _():
            for d in range(TP - 1):
                for k in range(PER):
                    got_right(d, g * PER + k).wait_recv()

        @pl.when(z == 0)
        def _():
            for d in range(TP - 1):
                for k in range(PER):
                    got_left(d, g * PER + k).wait_recv()

    def drain():
        def body(c, _):
            for d in range(TP - 1):
                @pl.when((z < TP - 1) & (z >= d))
                def _():
                    right(d, c).wait_send()

                @pl.when((z > 0) & (z + d <= TP - 1))
                def _():
                    left(d, c).wait_send()
            return 0
        lax.fori_loop(0, NCC, body, 0)

    return tick, arrived, drain


def norm_into(z, x_ref, gain_ref, bg):
    gain = gain_ref[...].reshape(1, DIM).astype(F32)

    def body(i, _):
        r0 = pl.multiple_of(i * 16, 16)
        wide = x_ref[pl.ds(r0, 16), :].astype(F32)
        inv = lax.rsqrt(jnp.mean(wide * wide, axis=-1, keepdims=True) + NORM_EPS)
        out = (wide * inv * gain).astype(BF16)
        row = pl.multiple_of(z * ROWS + r0, 16)
        for g in range(NK):
            bg[g, pl.ds(row, 16), :] = out[:, g * KC:(g + 1) * KC]
        return 0
    lax.fori_loop(0, ROWS // 16, body, 0)


GATHER_SEMS = [pltpu.SemaphoreType.DMA((TP - 1, NCC))] * 4

QT = 2304
SLOTS = 3
FINAL = 3
MID_HOP = 1
LAG = 8
AG_AT = 0


def mid_kernel(n_tiles, o_ref, x_ref, gain_ref, wo, wg, wu, out, h_ref, bg, part, from_left, from_right, acc, wbuf, wobuf, norm_b, ss, ratio,
               wsem, wosem, osem, r_right, r_left, s_right, s_left, p_right, p_left, p_send):
    z = lax.axis_index("tp")
    total = NK * 2 * n_tiles

    def fetch(i, start):
        q = i % (2 * n_tiles)
        k0 = pl.multiple_of((i // (2 * n_tiles)) * KC, KC)
        n0 = pl.multiple_of((q % n_tiles) * QT, QT)
        slot = i % SLOTS

        @pl.when(q < n_tiles)
        def _():
            c = pltpu.make_async_copy(wg.at[pl.ds(k0, KC), pl.ds(n0, QT)], wbuf.at[slot], wsem.at[slot])
            c.start() if start else c.wait()

        @pl.when(q >= n_tiles)
        def _():
            c = pltpu.make_async_copy(wu.at[pl.ds(k0, KC), pl.ds(n0, QT)], wbuf.at[slot], wsem.at[slot])
            c.start() if start else c.wait()

    def fetch_out(c):
        return pltpu.make_async_copy(wo.at[:, pl.ds(pl.multiple_of(c * CC, CC), CC)], wobuf.at[c % 2], wosem.at[c % 2])

    def send_right(c, dest):
        return pltpu.make_async_remote_copy(part.at[c, dest], from_left.at[c, dest - 1], p_send.at[c, dest], p_right.at[c, dest - 1],
                                            device_id={"tp": jnp.minimum(z + 1, TP - 1)}, device_id_type=MESH)

    def send_left(c, dest):
        return pltpu.make_async_remote_copy(part.at[c, dest], from_right.at[c, dest], p_send.at[c, dest], p_left.at[c, dest],
                                            device_id={"tp": jnp.maximum(z - 1, 0)}, device_id_type=MESH)

    def got_left(c, dest):
        return pltpu.make_async_remote_copy(part.at[c, dest], from_left.at[c, dest - 1], p_send.at[c, dest], p_right.at[c, dest - 1],
                                            device_id={"tp": jnp.maximum(z - 1, 0)}, device_id_type=MESH)

    def got_right(c, dest):
        return pltpu.make_async_remote_copy(part.at[c, dest], from_right.at[c, dest], p_send.at[c, dest], p_left.at[c, dest],
                                            device_id={"tp": jnp.minimum(z + 1, TP - 1)}, device_id_type=MESH)

    tp_signal(z)
    fetch_out(0).start()
    fetch_out(1).start()
    for i in range(SLOTS - 1):
        fetch(i, True)
    tick, arrived, drain_gather = gather_tools(z, MID_HOP, bg, r_right, r_left, s_right, s_left)

    def product(t):
        @pl.when(t < NCC)
        def _():
            fetch_out(t).wait()
            prod = jnp.dot(o_ref[...], wobuf[t % 2], preferred_element_type=F32).astype(BF16)
            for dest in range(TP):
                part[t, dest] = prod[dest * ROWS:(dest + 1) * ROWS]

            @pl.when(t + 2 < NCC)
            def _():
                fetch_out(t + 2).start()

    def scatter(t):
        cr = t - z
        ok_r = (cr >= 0) & (cr < NCC)
        cl = t - (TP - 1 - z)
        ok_l = (cl >= 0) & (cl < NCC)
        for k in range(TP - 1):
            dest = TP - 1 - k

            @pl.when(ok_r & (dest > z))
            def _():
                @pl.when(z > 0)
                def _():
                    got_left(cr, dest).wait_recv()
                    part[cr, dest] = (part[cr, dest].astype(F32) + from_left[cr, dest - 1].astype(F32)).astype(BF16)
                send_right(cr, dest).start()

            dst = k

            @pl.when(ok_l & (dst < z))
            def _():
                @pl.when(z < TP - 1)
                def _():
                    got_right(cl, dst).wait_recv()
                    part[cl, dst] = (part[cl, dst].astype(F32) + from_right[cl, dst].astype(F32)).astype(BF16)
                send_left(cl, dst).start()

        cf = t - FINAL

        @pl.when((cf >= 0) & (cf < NCC))
        def _():
            cols = pl.ds(pl.multiple_of(jnp.maximum(cf, 0) * CC, CC), CC)

            @pl.when(z > 0)
            def _():
                got_left(cf, z).wait_recv()
                part[cf, z] = (part[cf, z].astype(F32) + from_left[cf, z - 1].astype(F32)).astype(BF16)

            @pl.when(z < TP - 1)
            def _():
                got_right(cf, z).wait_recv()
                part[cf, z] = (part[cf, z].astype(F32) + from_right[cf, z].astype(F32)).astype(BF16)
            h = (x_ref[:, cols].astype(F32) + part[cf, z].astype(F32)).astype(BF16)
            h_ref[:, cols] = h
            lane = pl.multiple_of((cf % PER) * CC, CC)
            bg[cf // PER, pl.ds(pl.multiple_of(z * ROWS, ROWS), ROWS), pl.ds(lane, CC)] = h

    def normalize(g):
        gain = gain_ref[pl.ds(pl.multiple_of(g * KC, KC), KC)].reshape(1, KC).astype(F32)

        def body(i, _):
            rows = pl.ds(pl.multiple_of(i * ROWS, ROWS), ROWS)
            wide = bg[g, rows, :].astype(F32)
            old = ss[rows, :]
            new = old + jnp.sum(wide * wide, axis=-1, keepdims=True)
            r_old = lax.rsqrt(old / DIM + NORM_EPS)
            r_new = lax.rsqrt(new / DIM + NORM_EPS)
            ss[rows, :] = new
            ratio[rows, :] = jnp.where(r_old > 0.0, r_new / r_old, 0.0)
            norm_b[rows, :] = (wide * r_new[:, :1] * gain).astype(BF16)
            return 0
        lax.fori_loop(0, TP, body, 0)

    ss[...] = jnp.zeros(ss.shape, F32)
    product(0)
    tp_wait()

    def fill(t, _):
        @pl.when(t > 0)
        def _():
            product(t)
        scatter(t)
        tick(t - FINAL)

        @pl.when(t < 2 * n_tiles)
        def _():
            def zero(i, _):
                acc[t, pl.ds(pl.multiple_of(i * 32, 32), 32), :] = jnp.zeros((32, QT), F32)
                return 0
            lax.fori_loop(0, TP * ROWS // 32, zero, 0)
        return 0
    lax.fori_loop(0, LAG, fill, 0)

    def step(u, _):
        t = u + LAG
        g = u // 2
        product(t)
        scatter(t)

        @pl.when(u % 2 == 0)
        def _():
            arrived(g)
            normalize(g)

        def tile(j, _):
            i = u * n_tiles + j
            fetch(i, False)

            @pl.when(i + SLOTS - 1 < total)
            def _():
                fetch(i + SLOTS - 1, True)
            q = i % (2 * n_tiles)
            scale = jnp.concatenate([ratio[...]] * (QT // 128), axis=1)
            acc[q] = acc[q] * scale + jnp.dot(norm_b[...], wbuf[i % SLOTS], preferred_element_type=F32)

            @pl.when(j == AG_AT)
            def _():
                tick(t - FINAL)
            return 0
        lax.fori_loop(0, n_tiles, tile, 0)
        return 0
    lax.fori_loop(0, 2 * NK, step, 0)

    def put(j):
        return pltpu.make_async_copy(wbuf.at[j], out.at[:, pl.ds(j * QT, QT)], osem.at[j])

    for j in range(n_tiles):
        def finish(i, _):
            rows = pl.ds(pl.multiple_of(i * 64, 64), 64)
            wbuf[j, rows, :] = (jax.nn.silu(acc[j, rows, :]) * acc[n_tiles + j, rows, :]).astype(BF16)
            return 0
        lax.fori_loop(0, TP * ROWS // 64, finish, 0)
        put(j).start()
    drain_gather()

    def drain(c, _):
        for dest in range(TP):
            @pl.when(dest > z)
            def _():
                send_right(c, max(dest, 1)).wait_send()

            @pl.when(dest < z)
            def _():
                send_left(c, min(dest, TP - 2)).wait_send()
        return 0
    lax.fori_loop(0, NCC, drain, 0)
    for j in range(n_tiles):
        put(j).wait()


def mid(o, x, gain, wo, wg, wu):
    ffn = wg.shape[1]
    n_tiles = ffn // QT
    vm = pl.BlockSpec(memory_space=pltpu.VMEM)
    hbm = pl.BlockSpec(memory_space=pl.ANY)
    dma = pltpu.SemaphoreType.DMA
    return pl.pallas_call(
        functools.partial(mid_kernel, n_tiles),
        out_shape=(jax.ShapeDtypeStruct((TP * ROWS, ffn), BF16), jax.ShapeDtypeStruct((ROWS, DIM), BF16)),
        in_specs=[vm, vm, vm, hbm, hbm, hbm],
        out_specs=(hbm, vm),
        scratch_shapes=[
            pltpu.VMEM((NK, TP * ROWS, KC), BF16),
            pltpu.VMEM((NCC, TP, ROWS, CC), BF16),
            pltpu.VMEM((NCC, TP - 1, ROWS, CC), BF16),
            pltpu.VMEM((NCC, TP - 1, ROWS, CC), BF16),
            pltpu.VMEM((2 * n_tiles, TP * ROWS, QT), F32),
            pltpu.VMEM((SLOTS, KC, QT), BF16),
            pltpu.VMEM((2, wo.shape[0], CC), BF16),
            pltpu.VMEM((TP * ROWS, KC), BF16),
            pltpu.VMEM((TP * ROWS, 128), F32),
            pltpu.VMEM((TP * ROWS, 128), F32),
            dma((SLOTS,)), dma((2,)), dma((n_tiles,)),
        ] + GATHER_SEMS + [dma((NCC, TP - 1)), dma((NCC, TP - 1)), dma((NCC, TP))],
        compiler_params=pltpu.CompilerParams(collective_id=2, has_side_effects=True, vmem_limit_bytes=VMEM_LIMIT),
        name="out_gate_up",
    )(o, x, gain, wo, wg, wu)


def qkv_kernel(x_ref, gain_ref, pos_ref, freq_ref, wq, wk, wv, q_out, kv_out, pos_out,
               bg, acc, wbuf, pos_all, cos_t, sin_t, wsem, psend, precv, r_right, r_left, s_right, s_left):
    z = lax.axis_index("tp")
    nq, nkv = wq.shape[1], wk.shape[1]

    def fetch(g, start):
        k0 = pl.multiple_of(g * KC, KC)
        slot = g % 2
        for idx, (w, off, width) in enumerate(((wq, 0, nq), (wk, nq, nkv), (wv, nq + nkv, nkv))):
            c = pltpu.make_async_copy(w.at[pl.ds(k0, KC), :], wbuf.at[slot, :, pl.ds(off, width)], wsem.at[slot, idx])
            c.start() if start else c.wait()

    tp_signal(z)
    fetch(0, True)
    fetch(1, True)
    pos_all[z] = jnp.broadcast_to(pos_ref[...].reshape(1, ROWS), (8, ROWS))
    norm_into(z, x_ref, gain_ref, bg)
    tp_wait()
    tick, arrived, drain = gather_tools(z, HOP, bg, r_right, r_left, s_right, s_left)

    def pos_copy(peer, origin):
        return pltpu.make_async_remote_copy(pos_all.at[z], pos_all.at[origin], psend.at[peer], precv.at[origin],
                                            device_id={"tp": peer}, device_id_type=MESH)
    tick(0)
    for peer in range(TP):
        @pl.when(z != peer)
        def _():
            pos_copy(peer, z).start()
    acc[...] = jnp.zeros(acc.shape, F32)
    for t in range(1, FILL):
        tick(t)
    for peer in range(TP):
        @pl.when(z != peer)
        def _():
            pos_copy(peer, z).wait_send()
            pos_copy(peer, peer).wait_recv()
    lane = lax.broadcasted_iota(jnp.int32, (ROWS, HEAD_DIM), 1)
    for t in range(TP):
        wide = jnp.broadcast_to(pos_all[t, 0:1, :].astype(F32), (ROWS, ROWS)).T
        ang = wide * freq_ref[...]
        sin = jnp.sin(ang)
        cos_t[t * ROWS:(t + 1) * ROWS, :] = jnp.cos(ang)
        sin_t[t * ROWS:(t + 1) * ROWS, :] = jnp.where(lane < HEAD_DIM // 2, -sin, sin)
        ints = wide.astype(jnp.int32)
        for half in range(2):
            pos_out[half, t * PIECE:(t + 1) * PIECE, :] = ints[half * PIECE:(half + 1) * PIECE, :]

    def step(g, _):
        for h in range(2):
            tick(g * 2 + h + FILL)
        arrived(g)
        fetch(g, False)
        acc[...] += jnp.dot(bg[g], wbuf[g % 2], preferred_element_type=F32)

        @pl.when(g + 2 < NK)
        def _():
            fetch(g + 2, True)
        return 0
    lax.fori_loop(0, NK, step, 0)
    n_rope = (nq + nkv) // HEAD_DIM
    for head in range((nq + 2 * nkv) // HEAD_DIM):
        val = acc[:, head * HEAD_DIM:(head + 1) * HEAD_DIM]
        if head < n_rope:
            val = val * cos_t[...] + pltpu.roll(val, HEAD_DIM // 2, 1) * sin_t[...]
        val = val.astype(BF16)
        dst, idx = (q_out, head) if head < nq // HEAD_DIM else (kv_out, head - nq // HEAD_DIM)
        for t in range(TP):
            for half in range(2):
                r0 = t * ROWS + half * PIECE
                dst[idx, half, t * PIECE:(t + 1) * PIECE, :] = val[r0:r0 + PIECE, :]
    drain()


def qkv_proj(x, gain, pos, wq, wk, wv):
    width = wq.shape[1] + wk.shape[1] + wv.shape[1]
    nq, nkv = wq.shape[1] // HEAD_DIM, 2 * wk.shape[1] // HEAD_DIM
    vm = pl.BlockSpec(memory_space=pltpu.VMEM)
    hbm = pl.BlockSpec(memory_space=pl.ANY)
    half = HEAD_DIM // 2
    inv_freq = ROPE_BASE ** (-jnp.arange(half, dtype=F32) * (2.0 / HEAD_DIM))
    freq = jnp.concatenate([inv_freq, inv_freq]).reshape(1, HEAD_DIM)
    return pl.pallas_call(
        qkv_kernel,
        out_shape=(jax.ShapeDtypeStruct((nq, 2, TP * PIECE, HEAD_DIM), BF16), jax.ShapeDtypeStruct((nkv, 2, TP * PIECE, HEAD_DIM), BF16),
                   jax.ShapeDtypeStruct((2, TP * PIECE, HEAD_DIM), jnp.int32)),
        in_specs=[vm, vm, vm, vm, hbm, hbm, hbm],
        out_specs=(vm, vm, vm),
        scratch_shapes=[
            pltpu.VMEM((NK, TP * ROWS, KC), BF16),
            pltpu.VMEM((TP * ROWS, width), F32),
            pltpu.VMEM((2, KC, width), BF16),
            pltpu.VMEM((TP, 8, ROWS), jnp.int32),
            pltpu.VMEM((TP * ROWS, HEAD_DIM), F32),
            pltpu.VMEM((TP * ROWS, HEAD_DIM), F32),
            pltpu.SemaphoreType.DMA((2, 3)),
            pltpu.SemaphoreType.DMA((TP,)),
            pltpu.SemaphoreType.DMA((TP,)),
        ] + GATHER_SEMS,
        compiler_params=pltpu.CompilerParams(collective_id=1, has_side_effects=True, vmem_limit_bytes=VMEM_LIMIT),
        name="qkv_proj",
    )(x, gain, pos, freq, wq, wk, wv)


CP = 4
BLK = TP * PIECE
PIECES = 2 * CP * TP


def attend_kernel(q_ref, kv_ref, pos_ref, out_ref, kv_all, bias, m_ref, l_ref, acc, ssem, rsem):
    c = lax.axis_index("cp")
    heads = q_ref.shape[0]
    n_kv = kv_ref.shape[0] // 2
    group = heads // n_kv
    mate = c + 1 - 2 * (c % 2)
    across = (c + 2) % CP
    barrier = pltpu.get_barrier_semaphore()
    for peer in (mate, across):
        pl.semaphore_signal(barrier, inc=1, device_id={"cp": peer}, device_id_type=MESH)
    pl.semaphore_wait(barrier, 2)

    def send(src, block, peer, k):
        return pltpu.make_async_remote_copy(src, kv_all.at[block], ssem.at[k], rsem.at[k], device_id={"cp": peer}, device_id_type=MESH)

    to_across = send(kv_ref, c, across, 0)
    to_mate = send(kv_ref, c, mate, 1)
    to_across.start()
    to_mate.start()
    kv_all[c] = kv_ref[...]
    m_ref[...] = jnp.full(m_ref.shape, NEG_BIG, F32)
    l_ref[...] = jnp.zeros(l_ref.shape, F32)
    acc[...] = jnp.zeros(acc.shape, F32)

    def logical(idx, owner, half):
        early = owner * BLK + idx
        late = (PIECES - 1 - TP * owner - idx // PIECE) * PIECE + idx % PIECE
        return jnp.where(half == 0, early, late)

    def stage(i, _):
        src = jnp.where(i == 0, c, jnp.where(i == 1, mate, jnp.where(i == 2, across, CP - 1 - c)))

        @pl.when(i == 1)
        def _():
            send(kv_ref, mate, mate, 1).wait_recv()

        @pl.when(i == 2)
        def _():
            send(kv_ref, across, across, 0).wait_recv()
            send(kv_all.at[across], across, mate, 2).start()

        @pl.when(i == 3)
        def _():
            send(kv_all.at[across], CP - 1 - c, mate, 2).wait_recv()

        def job(j, _):
            qh = jnp.minimum(j, 1)
            kh = j // 2
            need = (j == 1) | ((j == 0) & (src <= c)) | ((j == 2) & (src >= c))

            @pl.when(need)
            def _():
                row = logical(lax.broadcasted_iota(jnp.int32, (BLK, BLK), 0), c, qh)
                col = logical(lax.broadcasted_iota(jnp.int32, (BLK, BLK), 1), src, kh)
                pos = pos_ref[qh]
                first = row - jnp.concatenate([pos, pos], axis=1)
                bias[...] = jnp.where((col <= row) & (col >= first), 0.0, NEG_BIG)

                def one(h, _):
                    g = h // group
                    s = lax.dot_general(q_ref[h, qh], kv_all[src, g, kh], (((1,), (1,)), ((), ())), preferred_element_type=F32)
                    s = s * (HEAD_DIM ** -0.5) + bias[...]
                    m_old = m_ref[qh, h]
                    m_new = jnp.maximum(m_old, jnp.max(s, axis=1, keepdims=True))
                    e = jnp.exp(s - jnp.concatenate([m_new, m_new], axis=1))
                    fac = jnp.exp(m_old - m_new)
                    m_ref[qh, h] = m_new
                    l_ref[qh, h] = l_ref[qh, h] * fac + jnp.sum(e, axis=1, keepdims=True)
                    acc[qh, h] = acc[qh, h] * fac + jnp.dot(e.astype(BF16), kv_all[src, n_kv + g, kh], preferred_element_type=F32)
                    return 0
                lax.fori_loop(0, heads, one, 0, unroll=UNROLL)
            return 0
        lax.fori_loop(0, 3, job, 0)
        return 0
    lax.fori_loop(0, CP, stage, 0)
    for h in range(heads):
        for half in range(2):
            o = (acc[half, h] / l_ref[half, h]).astype(BF16)
            for t in range(TP):
                r0 = t * ROWS + half * PIECE
                out_ref[r0:r0 + PIECE, h * HEAD_DIM:(h + 1) * HEAD_DIM] = o[t * PIECE:(t + 1) * PIECE, :]
    to_across.wait_send()
    to_mate.wait_send()
    send(kv_all.at[across], across, mate, 2).wait_send()


UNROLL = 10


def attend(q, kv, pos):
    heads = q.shape[0]
    vm = pl.BlockSpec(memory_space=pltpu.VMEM)
    state = pltpu.VMEM((2, heads, BLK, HEAD_DIM), F32)
    return pl.pallas_call(
        attend_kernel,
        out_shape=jax.ShapeDtypeStruct((TP * ROWS, heads * HEAD_DIM), BF16),
        in_specs=[vm, vm, vm],
        out_specs=vm,
        scratch_shapes=[pltpu.VMEM((CP,) + kv.shape, BF16), pltpu.VMEM((BLK, BLK), F32), state, state, state,
                        pltpu.SemaphoreType.DMA((3,)), pltpu.SemaphoreType.DMA((3,))],
        compiler_params=pltpu.CompilerParams(collective_id=5, has_side_effects=True, vmem_limit_bytes=VMEM_LIMIT),
        name="attend",
    )(q, kv, pos)


NC = 256
NN = DIM // NC
DOWN_FINAL = 5


def scatter_kernel(lhs, w, res_ref, out_ref, part, from_left, from_right, wbuf, wsem, r_right, r_left, ssem):
    z = lax.axis_index("tp")

    def fetch(c):
        return pltpu.make_async_copy(w.at[:, pl.ds(pl.multiple_of(c * NC, NC), NC)], wbuf.at[c % 2], wsem.at[c % 2])

    tp_signal(z)
    fetch(0).start()
    fetch(1).start()

    def send_right(c, dest):
        return pltpu.make_async_remote_copy(part.at[c, dest], from_left.at[c, dest - 1], ssem.at[c, dest], r_right.at[c, dest - 1],
                                            device_id={"tp": jnp.minimum(z + 1, TP - 1)}, device_id_type=MESH)

    def send_left(c, dest):
        return pltpu.make_async_remote_copy(part.at[c, dest], from_right.at[c, dest], ssem.at[c, dest], r_left.at[c, dest],
                                            device_id={"tp": jnp.maximum(z - 1, 0)}, device_id_type=MESH)

    def got_left(c, dest):
        return pltpu.make_async_remote_copy(part.at[c, dest], from_left.at[c, dest - 1], ssem.at[c, dest], r_right.at[c, dest - 1],
                                            device_id={"tp": jnp.maximum(z - 1, 0)}, device_id_type=MESH)

    def got_right(c, dest):
        return pltpu.make_async_remote_copy(part.at[c, dest], from_right.at[c, dest], ssem.at[c, dest], r_left.at[c, dest],
                                            device_id={"tp": jnp.minimum(z + 1, TP - 1)}, device_id_type=MESH)

    def product(t):
        @pl.when(t < NN)
        def _():
            fetch(t).wait()
            prod = jnp.dot(lhs[...], wbuf[t % 2], preferred_element_type=F32).astype(BF16)
            for dest in range(TP):
                part[t, dest] = prod[dest * ROWS:(dest + 1) * ROWS]

            @pl.when(t + 2 < NN)
            def _():
                fetch(t + 2).start()

    product(0)
    tp_wait()

    def step(t, _):
        @pl.when(t > 0)
        def _():
            product(t)

        cr = t - z
        ok_r = (cr >= 0) & (cr < NN)
        cl = t - (TP - 1 - z)
        ok_l = (cl >= 0) & (cl < NN)
        for k in range(TP - 1):
            dest = TP - 1 - k

            @pl.when(ok_r & (dest > z))
            def _():
                @pl.when(z > 0)
                def _():
                    got_left(cr, dest).wait_recv()
                    part[cr, dest] = (part[cr, dest].astype(F32) + from_left[cr, dest - 1].astype(F32)).astype(BF16)
                send_right(cr, dest).start()

            dst = k

            @pl.when(ok_l & (dst < z))
            def _():
                @pl.when(z < TP - 1)
                def _():
                    got_right(cl, dst).wait_recv()
                    part[cl, dst] = (part[cl, dst].astype(F32) + from_right[cl, dst].astype(F32)).astype(BF16)
                send_left(cl, dst).start()

        cf = t - DOWN_FINAL

        @pl.when(cf >= 0)
        def _():
            cols = pl.ds(pl.multiple_of(jnp.maximum(cf, 0) * NC, NC), NC)

            @pl.when(z > 0)
            def _():
                got_left(cf, z).wait_recv()
                part[cf, z] = (part[cf, z].astype(F32) + from_left[cf, z - 1].astype(F32)).astype(BF16)

            @pl.when(z < TP - 1)
            def _():
                got_right(cf, z).wait_recv()
                part[cf, z] = (part[cf, z].astype(F32) + from_right[cf, z].astype(F32)).astype(BF16)
            out_ref[:, cols] = (res_ref[:, cols].astype(F32) + part[cf, z].astype(F32)).astype(BF16)
        return 0
    lax.fori_loop(0, NN + DOWN_FINAL, step, 0)

    def drain(c, _):
        for dest in range(TP):
            @pl.when(dest > z)
            def _():
                send_right(c, max(dest, 1)).wait_send()

            @pl.when(dest < z)
            def _():
                send_left(c, min(dest, TP - 2)).wait_send()
        return 0
    lax.fori_loop(0, NN, drain, 0)


def scatter_proj(lhs, w, res, cid, name):
    depth = w.shape[0]
    vm = pl.BlockSpec(memory_space=pltpu.VMEM)
    hbm = pl.BlockSpec(memory_space=pl.ANY)
    return pl.pallas_call(
        scatter_kernel,
        out_shape=jax.ShapeDtypeStruct((ROWS, DIM), BF16),
        in_specs=[vm, hbm, vm],
        out_specs=vm,
        scratch_shapes=[
            pltpu.VMEM((NN, TP, ROWS, NC), BF16),
            pltpu.VMEM((NN, TP - 1, ROWS, NC), BF16),
            pltpu.VMEM((NN, TP - 1, ROWS, NC), BF16),
            pltpu.VMEM((2, depth, NC), BF16),
            pltpu.SemaphoreType.DMA((2,)),
            pltpu.SemaphoreType.DMA((NN, TP - 1)),
            pltpu.SemaphoreType.DMA((NN, TP - 1)),
            pltpu.SemaphoreType.DMA((NN, TP)),
        ],
        compiler_params=pltpu.CompilerParams(collective_id=cid, has_side_effects=True, vmem_limit_bytes=VMEM_LIMIT),
        name=name,
    )(lhs, w, res)


def solution(mesh):
    row_mat = P(('dp', 'cp', 'tp'), None)
    row_vec = P(('dp', 'cp', 'tp'))
    col_split = P(None, 'tp')
    row_split = P('tp', None)

    def local_layer(hidden, positions, doc_ids, attn_gain, mlp_gain, w_query, w_key, w_value, w_out, w_gate, w_up, w_down):
        q, kv, pos = qkv_proj(hidden, attn_gain, positions, w_query, w_key, w_value)
        attn_mix = attend(q, kv, pos)
        gated, residual = mid(attn_mix, hidden, mlp_gain, w_out, w_gate, w_up)
        return scatter_proj(gated, w_down, residual, 4, "down_proj")

    in_specs = (row_mat, row_vec, row_vec, P(None), P(None), col_split, col_split, col_split, row_split, col_split, col_split, row_split)
    return jax.shard_map(local_layer, mesh=mesh, in_specs=in_specs, out_specs=row_mat, check_vma=False)
```

```python
import functools

import jax
import jax.numpy as jnp
from jax import lax
from jax.experimental import pallas as pl
from jax.experimental.pallas import tpu as pltpu
from jax.sharding import PartitionSpec as P

HEAD_DIM = 128
ROPE_BASE = 500000.0
NORM_EPS = 1e-5
NEG_BIG = -1e30
MESH = pl.DeviceIdType.MESH
BF16 = jnp.bfloat16
F32 = jnp.float32
VMEM_LIMIT = 67043328

TP = 4
ROWS = 128
DIM = 5120
KC = 512
NK = DIM // KC
CC = 256
NCC = DIM // CC
PER = KC // CC
HOP = 2
FILL = 2 * HOP + PER
PIECE = ROWS // 2


def tp_signal(z):
    barrier = pltpu.get_barrier_semaphore()
    for peer in range(TP):
        @pl.when(z != peer)
        def _():
            pl.semaphore_signal(barrier, inc=1, device_id={"tp": peer}, device_id_type=MESH)


def tp_wait():
    pl.semaphore_wait(pltpu.get_barrier_semaphore(), TP - 1)


def gather_tools(z, hop, bg, r_right, r_left, s_right, s_left):
    def blk(origin, chunk):
        lane = pl.multiple_of((chunk % PER) * CC, CC)
        return bg.at[chunk // PER, pl.ds(pl.multiple_of(origin * ROWS, ROWS), ROWS), pl.ds(lane, CC)]

    def right(dist, chunk):
        ref = blk(z - dist, chunk)
        return pltpu.make_async_remote_copy(ref, ref, s_right.at[dist, chunk], r_right.at[dist, chunk],
                                            device_id={"tp": jnp.minimum(z + 1, TP - 1)}, device_id_type=MESH)

    def left(dist, chunk):
        ref = blk(z + dist, chunk)
        return pltpu.make_async_remote_copy(ref, ref, s_left.at[dist, chunk], r_left.at[dist, chunk],
                                            device_id={"tp": jnp.maximum(z - 1, 0)}, device_id_type=MESH)

    def got_right(dist, chunk):
        ref = blk(z - 1 - dist, chunk)
        return pltpu.make_async_remote_copy(ref, ref, s_right.at[dist, chunk], r_right.at[dist, chunk],
                                            device_id={"tp": jnp.maximum(z - 1, 0)}, device_id_type=MESH)

    def got_left(dist, chunk):
        ref = blk(z + 1 + dist, chunk)
        return pltpu.make_async_remote_copy(ref, ref, s_left.at[dist, chunk], r_left.at[dist, chunk],
                                            device_id={"tp": jnp.minimum(z + 1, TP - 1)}, device_id_type=MESH)

    def tick(t):
        own = (t >= 0) & (t < NCC)

        @pl.when(own & (z < TP - 1))
        def _():
            right(0, t).start()

        @pl.when(own & (z > 0))
        def _():
            left(0, t).start()

        for d in (1, 2):
            c = t - d * hop
            ok = (c >= 0) & (c < NCC)

            @pl.when(ok & (z < TP - 1) & (z >= d))
            def _():
                got_right(d - 1, c).wait_recv()
                right(d, c).start()

            @pl.when(ok & (z > 0) & (z + d <= TP - 1))
            def _():
                got_left(d - 1, c).wait_recv()
                left(d, c).start()

    def arrived(g):
        @pl.when(z == TP - 1)
        def _():
            for d in range(TP - 1):
                for k in range(PER):
                    got_right(d, g * PER + k).wait_recv()

        @pl.when(z == 0)
        def _():
            for d in range(TP - 1):
                for k in range(PER):
                    got_left(d, g * PER + k).wait_recv()

    def drain():
        def body(c, _):
            for d in range(TP - 1):
                @pl.when((z < TP - 1) & (z >= d))
                def _():
                    right(d, c).wait_send()

                @pl.when((z > 0) & (z + d <= TP - 1))
                def _():
                    left(d, c).wait_send()
            return 0
        lax.fori_loop(0, NCC, body, 0)

    return tick, arrived, drain


def norm_into(z, x_ref, gain_ref, bg):
    gain = gain_ref[...].reshape(1, DIM).astype(F32)

    def body(i, _):
        r0 = pl.multiple_of(i * 16, 16)
        wide = x_ref[pl.ds(r0, 16), :].astype(F32)
        inv = lax.rsqrt(jnp.mean(wide * wide, axis=-1, keepdims=True) + NORM_EPS)
        out = (wide * inv * gain).astype(BF16)
        row = pl.multiple_of(z * ROWS + r0, 16)
        for g in range(NK):
            bg[g, pl.ds(row, 16), :] = out[:, g * KC:(g + 1) * KC]
        return 0
    lax.fori_loop(0, ROWS // 16, body, 0)


GATHER_SEMS = [pltpu.SemaphoreType.DMA((TP - 1, NCC))] * 4

QT = 2304
SLOTS = 3
FINAL = 3
MID_HOP = 1
LAG = 8
AG_AT = 0


def mid_kernel(n_tiles, o_ref, x_ref, gain_ref, wo, wg, wu, out, h_ref, bg, part, from_left, from_right, acc, wbuf, wobuf, norm_b, ss, ratio,
               wsem, wosem, osem, r_right, r_left, s_right, s_left, p_right, p_left, p_send):
    z = lax.axis_index("tp")
    total = NK * 2 * n_tiles

    def fetch(i, start):
        q = i % (2 * n_tiles)
        k0 = pl.multiple_of((i // (2 * n_tiles)) * KC, KC)
        n0 = pl.multiple_of((q % n_tiles) * QT, QT)
        slot = i % SLOTS

        @pl.when(q < n_tiles)
        def _():
            c = pltpu.make_async_copy(wg.at[pl.ds(k0, KC), pl.ds(n0, QT)], wbuf.at[slot], wsem.at[slot])
            c.start() if start else c.wait()

        @pl.when(q >= n_tiles)
        def _():
            c = pltpu.make_async_copy(wu.at[pl.ds(k0, KC), pl.ds(n0, QT)], wbuf.at[slot], wsem.at[slot])
            c.start() if start else c.wait()

    def fetch_out(c):
        return pltpu.make_async_copy(wo.at[:, pl.ds(pl.multiple_of(c * CC, CC), CC)], wobuf.at[c % 2], wosem.at[c % 2])

    def send_right(c, dest):
        return pltpu.make_async_remote_copy(part.at[c, dest], from_left.at[c, dest - 1], p_send.at[c, dest], p_right.at[c, dest - 1],
                                            device_id={"tp": jnp.minimum(z + 1, TP - 1)}, device_id_type=MESH)

    def send_left(c, dest):
        return pltpu.make_async_remote_copy(part.at[c, dest], from_right.at[c, dest], p_send.at[c, dest], p_left.at[c, dest],
                                            device_id={"tp": jnp.maximum(z - 1, 0)}, device_id_type=MESH)

    def got_left(c, dest):
        return pltpu.make_async_remote_copy(part.at[c, dest], from_left.at[c, dest - 1], p_send.at[c, dest], p_right.at[c, dest - 1],
                                            device_id={"tp": jnp.maximum(z - 1, 0)}, device_id_type=MESH)

    def got_right(c, dest):
        return pltpu.make_async_remote_copy(part.at[c, dest], from_right.at[c, dest], p_send.at[c, dest], p_left.at[c, dest],
                                            device_id={"tp": jnp.minimum(z + 1, TP - 1)}, device_id_type=MESH)

    tp_signal(z)
    fetch_out(0).start()
    fetch_out(1).start()
    for i in range(SLOTS - 1):
        fetch(i, True)
    tick, arrived, drain_gather = gather_tools(z, MID_HOP, bg, r_right, r_left, s_right, s_left)

    def product(t):
        @pl.when(t < NCC)
        def _():
            fetch_out(t).wait()
            prod = jnp.dot(o_ref[...], wobuf[t % 2], preferred_element_type=F32).astype(BF16)
            for dest in range(TP):
                part[t, dest] = prod[dest * ROWS:(dest + 1) * ROWS]

            @pl.when(t + 2 < NCC)
            def _():
                fetch_out(t + 2).start()

    def scatter(t):
        cr = t - z
        ok_r = (cr >= 0) & (cr < NCC)
        cl = t - (TP - 1 - z)
        ok_l = (cl >= 0) & (cl < NCC)
        for k in range(TP - 1):
            dest = TP - 1 - k

            @pl.when(ok_r & (dest > z))
            def _():
                @pl.when(z > 0)
                def _():
                    got_left(cr, dest).wait_recv()
                    part[cr, dest] = (part[cr, dest].astype(F32) + from_left[cr, dest - 1].astype(F32)).astype(BF16)
                send_right(cr, dest).start()

            dst = k

            @pl.when(ok_l & (dst < z))
            def _():
                @pl.when(z < TP - 1)
                def _():
                    got_right(cl, dst).wait_recv()
                    part[cl, dst] = (part[cl, dst].astype(F32) + from_right[cl, dst].astype(F32)).astype(BF16)
                send_left(cl, dst).start()

        cf = t - FINAL

        @pl.when((cf >= 0) & (cf < NCC))
        def _():
            cols = pl.ds(pl.multiple_of(jnp.maximum(cf, 0) * CC, CC), CC)

            @pl.when(z > 0)
            def _():
                got_left(cf, z).wait_recv()
                part[cf, z] = (part[cf, z].astype(F32) + from_left[cf, z - 1].astype(F32)).astype(BF16)

            @pl.when(z < TP - 1)
            def _():
                got_right(cf, z).wait_recv()
                part[cf, z] = (part[cf, z].astype(F32) + from_right[cf, z].astype(F32)).astype(BF16)
            h = (x_ref[:, cols].astype(F32) + part[cf, z].astype(F32)).astype(BF16)
            h_ref[:, cols] = h
            lane = pl.multiple_of((cf % PER) * CC, CC)
            bg[cf // PER, pl.ds(pl.multiple_of(z * ROWS, ROWS), ROWS), pl.ds(lane, CC)] = h

    def normalize(g):
        gain = gain_ref[pl.ds(pl.multiple_of(g * KC, KC), KC)].reshape(1, KC).astype(F32)

        def body(i, _):
            rows = pl.ds(pl.multiple_of(i * ROWS, ROWS), ROWS)
            wide = bg[g, rows, :].astype(F32)
            old = ss[rows, :]
            new = old + jnp.sum(wide * wide, axis=-1, keepdims=True)
            r_old = lax.rsqrt(old / DIM + NORM_EPS)
            r_new = lax.rsqrt(new / DIM + NORM_EPS)
            ss[rows, :] = new
            ratio[rows, :] = jnp.where(r_old > 0.0, r_new / r_old, 0.0)
            norm_b[rows, :] = (wide * r_new[:, :1] * gain).astype(BF16)
            return 0
        lax.fori_loop(0, TP, body, 0)

    ss[...] = jnp.zeros(ss.shape, F32)
    product(0)
    tp_wait()

    def fill(t, _):
        scatter(t)
        product(t + 1)
        tick(t - FINAL)

        @pl.when(t < 2 * n_tiles)
        def _():
            def zero(i, _):
                acc[t, pl.ds(pl.multiple_of(i * 32, 32), 32), :] = jnp.zeros((32, QT), F32)
                return 0
            lax.fori_loop(0, TP * ROWS // 32, zero, 0)
        return 0
    lax.fori_loop(0, LAG, fill, 0)

    def step(u, _):
        t = u + LAG
        g = u // 2
        scatter(t)

        @pl.when(u % 2 == 0)
        def _():
            arrived(g)
            normalize(g)

        def tile(j, _):
            i = u * n_tiles + j
            fetch(i, False)

            @pl.when(i + SLOTS - 1 < total)
            def _():
                fetch(i + SLOTS - 1, True)
            q = i % (2 * n_tiles)
            scale = jnp.concatenate([ratio[...]] * (QT // 128), axis=1)
            acc[q] = acc[q] * scale + jnp.dot(norm_b[...], wbuf[i % SLOTS], preferred_element_type=F32)

            @pl.when(j == AG_AT)
            def _():
                tick(t - FINAL)
                product(t + 1)
            return 0
        lax.fori_loop(0, n_tiles, tile, 0)
        return 0
    lax.fori_loop(0, 2 * NK, step, 0)

    def put(j):
        return pltpu.make_async_copy(wbuf.at[j], out.at[:, pl.ds(j * QT, QT)], osem.at[j])

    for j in range(n_tiles):
        def finish(i, _):
            rows = pl.ds(pl.multiple_of(i * 64, 64), 64)
            wbuf[j, rows, :] = (jax.nn.silu(acc[j, rows, :]) * acc[n_tiles + j, rows, :]).astype(BF16)
            return 0
        lax.fori_loop(0, TP * ROWS // 64, finish, 0)
        put(j).start()
    drain_gather()

    def drain(c, _):
        for dest in range(TP):
            @pl.when(dest > z)
            def _():
                send_right(c, max(dest, 1)).wait_send()

            @pl.when(dest < z)
            def _():
                send_left(c, min(dest, TP - 2)).wait_send()
        return 0
    lax.fori_loop(0, NCC, drain, 0)
    for j in range(n_tiles):
        put(j).wait()


def mid(o, x, gain, wo, wg, wu):
    ffn = wg.shape[1]
    n_tiles = ffn // QT
    vm = pl.BlockSpec(memory_space=pltpu.VMEM)
    hbm = pl.BlockSpec(memory_space=pl.ANY)
    dma = pltpu.SemaphoreType.DMA
    return pl.pallas_call(
        functools.partial(mid_kernel, n_tiles),
        out_shape=(jax.ShapeDtypeStruct((TP * ROWS, ffn), BF16), jax.ShapeDtypeStruct((ROWS, DIM), BF16)),
        in_specs=[vm, vm, vm, hbm, hbm, hbm],
        out_specs=(hbm, vm),
        scratch_shapes=[
            pltpu.VMEM((NK, TP * ROWS, KC), BF16),
            pltpu.VMEM((NCC, TP, ROWS, CC), BF16),
            pltpu.VMEM((NCC, TP - 1, ROWS, CC), BF16),
            pltpu.VMEM((NCC, TP - 1, ROWS, CC), BF16),
            pltpu.VMEM((2 * n_tiles, TP * ROWS, QT), F32),
            pltpu.VMEM((SLOTS, KC, QT), BF16),
            pltpu.VMEM((2, wo.shape[0], CC), BF16),
            pltpu.VMEM((TP * ROWS, KC), BF16),
            pltpu.VMEM((TP * ROWS, 128), F32),
            pltpu.VMEM((TP * ROWS, 128), F32),
            dma((SLOTS,)), dma((2,)), dma((n_tiles,)),
        ] + GATHER_SEMS + [dma((NCC, TP - 1)), dma((NCC, TP - 1)), dma((NCC, TP))],
        compiler_params=pltpu.CompilerParams(collective_id=2, has_side_effects=True, vmem_limit_bytes=VMEM_LIMIT),
        name="out_gate_up",
    )(o, x, gain, wo, wg, wu)


def qkv_kernel(x_ref, gain_ref, pos_ref, freq_ref, wq, wk, wv, q_out, kv_out, pos_out,
               bg, acc, wbuf, pos_all, cos_t, sin_t, wsem, psend, precv, r_right, r_left, s_right, s_left):
    z = lax.axis_index("tp")
    nq, nkv = wq.shape[1], wk.shape[1]

    def fetch(g, start):
        k0 = pl.multiple_of(g * KC, KC)
        slot = g % 2
        for idx, (w, off, width) in enumerate(((wq, 0, nq), (wk, nq, nkv), (wv, nq + nkv, nkv))):
            c = pltpu.make_async_copy(w.at[pl.ds(k0, KC), :], wbuf.at[slot, :, pl.ds(off, width)], wsem.at[slot, idx])
            c.start() if start else c.wait()

    tp_signal(z)
    fetch(0, True)
    fetch(1, True)
    pos_all[z] = jnp.broadcast_to(pos_ref[...].reshape(1, ROWS), (8, ROWS))
    norm_into(z, x_ref, gain_ref, bg)
    tp_wait()
    tick, arrived, drain = gather_tools(z, HOP, bg, r_right, r_left, s_right, s_left)

    def pos_copy(peer, origin):
        return pltpu.make_async_remote_copy(pos_all.at[z], pos_all.at[origin], psend.at[peer], precv.at[origin],
                                            device_id={"tp": peer}, device_id_type=MESH)
    tick(0)
    for peer in range(TP):
        @pl.when(z != peer)
        def _():
            pos_copy(peer, z).start()
    acc[...] = jnp.zeros(acc.shape, F32)
    for t in range(1, FILL):
        tick(t)
    for peer in range(TP):
        @pl.when(z != peer)
        def _():
            pos_copy(peer, z).wait_send()
            pos_copy(peer, peer).wait_recv()
    lane = lax.broadcasted_iota(jnp.int32, (ROWS, HEAD_DIM), 1)
    for t in range(TP):
        wide = jnp.broadcast_to(pos_all[t, 0:1, :].astype(F32), (ROWS, ROWS)).T
        ang = wide * freq_ref[...]
        sin = jnp.sin(ang)
        cos_t[t * ROWS:(t + 1) * ROWS, :] = jnp.cos(ang)
        sin_t[t * ROWS:(t + 1) * ROWS, :] = jnp.where(lane < HEAD_DIM // 2, -sin, sin)
        ints = wide.astype(jnp.int32)
        for half in range(2):
            pos_out[half, t * PIECE:(t + 1) * PIECE, :] = ints[half * PIECE:(half + 1) * PIECE, :]

    def step(g, _):
        for h in range(2):
            tick(g * 2 + h + FILL)
        arrived(g)
        fetch(g, False)
        acc[...] += jnp.dot(bg[g], wbuf[g % 2], preferred_element_type=F32)

        @pl.when(g + 2 < NK)
        def _():
            fetch(g + 2, True)
        return 0
    lax.fori_loop(0, NK, step, 0)
    n_rope = (nq + nkv) // HEAD_DIM
    for head in range((nq + 2 * nkv) // HEAD_DIM):
        val = acc[:, head * HEAD_DIM:(head + 1) * HEAD_DIM]
        if head < n_rope:
            val = val * cos_t[...] + pltpu.roll(val, HEAD_DIM // 2, 1) * sin_t[...]
        val = val.astype(BF16)
        dst, idx = (q_out, head) if head < nq // HEAD_DIM else (kv_out, head - nq // HEAD_DIM)
        for t in range(TP):
            for half in range(2):
                r0 = t * ROWS + half * PIECE
                dst[idx, half, t * PIECE:(t + 1) * PIECE, :] = val[r0:r0 + PIECE, :]
    drain()


def qkv_proj(x, gain, pos, wq, wk, wv):
    width = wq.shape[1] + wk.shape[1] + wv.shape[1]
    nq, nkv = wq.shape[1] // HEAD_DIM, 2 * wk.shape[1] // HEAD_DIM
    vm = pl.BlockSpec(memory_space=pltpu.VMEM)
    hbm = pl.BlockSpec(memory_space=pl.ANY)
    half = HEAD_DIM // 2
    inv_freq = ROPE_BASE ** (-jnp.arange(half, dtype=F32) * (2.0 / HEAD_DIM))
    freq = jnp.concatenate([inv_freq, inv_freq]).reshape(1, HEAD_DIM)
    return pl.pallas_call(
        qkv_kernel,
        out_shape=(jax.ShapeDtypeStruct((nq, 2, TP * PIECE, HEAD_DIM), BF16), jax.ShapeDtypeStruct((nkv, 2, TP * PIECE, HEAD_DIM), BF16),
                   jax.ShapeDtypeStruct((2, TP * PIECE, HEAD_DIM), jnp.int32)),
        in_specs=[vm, vm, vm, vm, hbm, hbm, hbm],
        out_specs=(vm, vm, vm),
        scratch_shapes=[
            pltpu.VMEM((NK, TP * ROWS, KC), BF16),
            pltpu.VMEM((TP * ROWS, width), F32),
            pltpu.VMEM((2, KC, width), BF16),
            pltpu.VMEM((TP, 8, ROWS), jnp.int32),
            pltpu.VMEM((TP * ROWS, HEAD_DIM), F32),
            pltpu.VMEM((TP * ROWS, HEAD_DIM), F32),
            pltpu.SemaphoreType.DMA((2, 3)),
            pltpu.SemaphoreType.DMA((TP,)),
            pltpu.SemaphoreType.DMA((TP,)),
        ] + GATHER_SEMS,
        compiler_params=pltpu.CompilerParams(collective_id=1, has_side_effects=True, vmem_limit_bytes=VMEM_LIMIT),
        name="qkv_proj",
    )(x, gain, pos, freq, wq, wk, wv)


CP = 4
BLK = TP * PIECE
PIECES = 2 * CP * TP


def attend_kernel(q_ref, kv_ref, pos_ref, out_ref, kv_all, bias, m_ref, l_ref, acc, ssem, rsem):
    c = lax.axis_index("cp")
    heads = q_ref.shape[0]
    n_kv = kv_ref.shape[0] // 2
    group = heads // n_kv
    mate = c + 1 - 2 * (c % 2)
    across = (c + 2) % CP
    barrier = pltpu.get_barrier_semaphore()
    for peer in (mate, across):
        pl.semaphore_signal(barrier, inc=1, device_id={"cp": peer}, device_id_type=MESH)
    pl.semaphore_wait(barrier, 2)

    def half_copy(src, block, peer, half, k):
        return pltpu.make_async_remote_copy(src.at[:, half], kv_all.at[block, :, half], ssem.at[k], rsem.at[k],
                                            device_id={"cp": peer}, device_id_type=MESH)

    def mate_copy(block, peer):
        return pltpu.make_async_remote_copy(kv_ref, kv_all.at[block], ssem.at[4], rsem.at[4], device_id={"cp": peer}, device_id_type=MESH)

    def relay(half):
        return half_copy(kv_all.at[across], across, mate, half, 2 + half)

    for half in range(2):
        half_copy(kv_ref, c, across, half, half).start()
    mate_copy(c, mate).start()
    kv_all[c] = kv_ref[...]
    m_ref[...] = jnp.full(m_ref.shape, NEG_BIG, F32)
    l_ref[...] = jnp.zeros(l_ref.shape, F32)
    acc[...] = jnp.zeros(acc.shape, F32)

    def logical(idx, owner, half):
        early = owner * BLK + idx
        late = (PIECES - 1 - TP * owner - idx // PIECE) * PIECE + idx % PIECE
        return jnp.where(half == 0, early, late)

    def stage(i, _):
        diag = CP - 1 - c
        src = jnp.where(i == 0, c, jnp.where(i == 1, mate, jnp.where(i % 2 == 0, across, diag)))

        @pl.when(i == 1)
        def _():
            mate_copy(mate, mate).wait_recv()

        for half in range(2):
            @pl.when(i == 2 + 2 * half)
            def _():
                half_copy(kv_ref, across, across, half, half).wait_recv()
                relay(half).start()

            @pl.when(i == 3 + 2 * half)
            def _():
                half_copy(kv_all.at[across], diag, mate, half, 2 + half).wait_recv()

        def job(j, _):
            qh = jnp.minimum(j, 1)
            kh = j // 2
            early, late = i < CP, (i < 2) | (i >= CP)
            need = (early & (j == 1)) | (early & (j == 0) & (src <= c)) | (late & (j == 2) & (src >= c))

            @pl.when(need)
            def _():
                row = logical(lax.broadcasted_iota(jnp.int32, (BLK, BLK), 0), c, qh)
                col = logical(lax.broadcasted_iota(jnp.int32, (BLK, BLK), 1), src, kh)
                pos = pos_ref[qh]
                first = row - jnp.concatenate([pos, pos], axis=1)
                bias[...] = jnp.where((col <= row) & (col >= first), 0.0, NEG_BIG)

                def one(h, _):
                    g = h // group
                    s = lax.dot_general(q_ref[h, qh], kv_all[src, g, kh], (((1,), (1,)), ((), ())), preferred_element_type=F32)
                    s = s * (HEAD_DIM ** -0.5) + bias[...]
                    m_old = m_ref[qh, h]
                    m_new = jnp.maximum(m_old, jnp.max(s, axis=1, keepdims=True))
                    e = jnp.exp(s - jnp.concatenate([m_new, m_new], axis=1))
                    fac = jnp.exp(m_old - m_new)
                    m_ref[qh, h] = m_new
                    l_ref[qh, h] = l_ref[qh, h] * fac + jnp.sum(e, axis=1, keepdims=True)
                    acc[qh, h] = acc[qh, h] * fac + jnp.dot(e.astype(BF16), kv_all[src, n_kv + g, kh], preferred_element_type=F32)
                    return 0
                lax.fori_loop(0, heads, one, 0, unroll=UNROLL)
            return 0
        lax.fori_loop(0, 3, job, 0)
        return 0
    lax.fori_loop(0, CP + 2, stage, 0)
    for h in range(heads):
        for half in range(2):
            o = (acc[half, h] / l_ref[half, h]).astype(BF16)
            for t in range(TP):
                r0 = t * ROWS + half * PIECE
                out_ref[r0:r0 + PIECE, h * HEAD_DIM:(h + 1) * HEAD_DIM] = o[t * PIECE:(t + 1) * PIECE, :]
    for half in range(2):
        half_copy(kv_ref, c, across, half, half).wait_send()
        relay(half).wait_send()
    mate_copy(c, mate).wait_send()


UNROLL = 10


def attend(q, kv, pos):
    heads = q.shape[0]
    vm = pl.BlockSpec(memory_space=pltpu.VMEM)
    state = pltpu.VMEM((2, heads, BLK, HEAD_DIM), F32)
    return pl.pallas_call(
        attend_kernel,
        out_shape=jax.ShapeDtypeStruct((TP * ROWS, heads * HEAD_DIM), BF16),
        in_specs=[vm, vm, vm],
        out_specs=vm,
        scratch_shapes=[pltpu.VMEM((CP,) + kv.shape, BF16), pltpu.VMEM((BLK, BLK), F32), state, state, state,
                        pltpu.SemaphoreType.DMA((5,)), pltpu.SemaphoreType.DMA((5,))],
        compiler_params=pltpu.CompilerParams(collective_id=5, has_side_effects=True, vmem_limit_bytes=VMEM_LIMIT),
        name="attend",
    )(q, kv, pos)


NC = 256
NN = DIM // NC
DOWN_FINAL = 5


def scatter_kernel(lhs, w, res_ref, out_ref, part, from_left, from_right, wbuf, wsem, r_right, r_left, ssem):
    z = lax.axis_index("tp")

    def fetch(c):
        return pltpu.make_async_copy(w.at[:, pl.ds(pl.multiple_of(c * NC, NC), NC)], wbuf.at[c % 2], wsem.at[c % 2])

    tp_signal(z)
    fetch(0).start()
    fetch(1).start()

    def send_right(c, dest):
        return pltpu.make_async_remote_copy(part.at[c, dest], from_left.at[c, dest - 1], ssem.at[c, dest], r_right.at[c, dest - 1],
                                            device_id={"tp": jnp.minimum(z + 1, TP - 1)}, device_id_type=MESH)

    def send_left(c, dest):
        return pltpu.make_async_remote_copy(part.at[c, dest], from_right.at[c, dest], ssem.at[c, dest], r_left.at[c, dest],
                                            device_id={"tp": jnp.maximum(z - 1, 0)}, device_id_type=MESH)

    def got_left(c, dest):
        return pltpu.make_async_remote_copy(part.at[c, dest], from_left.at[c, dest - 1], ssem.at[c, dest], r_right.at[c, dest - 1],
                                            device_id={"tp": jnp.maximum(z - 1, 0)}, device_id_type=MESH)

    def got_right(c, dest):
        return pltpu.make_async_remote_copy(part.at[c, dest], from_right.at[c, dest], ssem.at[c, dest], r_left.at[c, dest],
                                            device_id={"tp": jnp.minimum(z + 1, TP - 1)}, device_id_type=MESH)

    def product(t):
        @pl.when(t < NN)
        def _():
            fetch(t).wait()
            prod = jnp.dot(lhs[...], wbuf[t % 2], preferred_element_type=F32).astype(BF16)
            for dest in range(TP):
                part[t, dest] = prod[dest * ROWS:(dest + 1) * ROWS]

            @pl.when(t + 2 < NN)
            def _():
                fetch(t + 2).start()

    product(0)
    tp_wait()

    def step(t, _):
        @pl.when(t > 0)
        def _():
            product(t)

        cr = t - z
        ok_r = (cr >= 0) & (cr < NN)
        cl = t - (TP - 1 - z)
        ok_l = (cl >= 0) & (cl < NN)
        for k in range(TP - 1):
            dest = TP - 1 - k

            @pl.when(ok_r & (dest > z))
            def _():
                @pl.when(z > 0)
                def _():
                    got_left(cr, dest).wait_recv()
                    part[cr, dest] = (part[cr, dest].astype(F32) + from_left[cr, dest - 1].astype(F32)).astype(BF16)
                send_right(cr, dest).start()

            dst = k

            @pl.when(ok_l & (dst < z))
            def _():
                @pl.when(z < TP - 1)
                def _():
                    got_right(cl, dst).wait_recv()
                    part[cl, dst] = (part[cl, dst].astype(F32) + from_right[cl, dst].astype(F32)).astype(BF16)
                send_left(cl, dst).start()

        cf = t - DOWN_FINAL

        @pl.when(cf >= 0)
        def _():
            cols = pl.ds(pl.multiple_of(jnp.maximum(cf, 0) * NC, NC), NC)

            @pl.when(z > 0)
            def _():
                got_left(cf, z).wait_recv()
                part[cf, z] = (part[cf, z].astype(F32) + from_left[cf, z - 1].astype(F32)).astype(BF16)

            @pl.when(z < TP - 1)
            def _():
                got_right(cf, z).wait_recv()
                part[cf, z] = (part[cf, z].astype(F32) + from_right[cf, z].astype(F32)).astype(BF16)
            out_ref[:, cols] = (res_ref[:, cols].astype(F32) + part[cf, z].astype(F32)).astype(BF16)
        return 0
    lax.fori_loop(0, NN + DOWN_FINAL, step, 0)

    def drain(c, _):
        for dest in range(TP):
            @pl.when(dest > z)
            def _():
                send_right(c, max(dest, 1)).wait_send()

            @pl.when(dest < z)
            def _():
                send_left(c, min(dest, TP - 2)).wait_send()
        return 0
    lax.fori_loop(0, NN, drain, 0)


def scatter_proj(lhs, w, res, cid, name):
    depth = w.shape[0]
    vm = pl.BlockSpec(memory_space=pltpu.VMEM)
    hbm = pl.BlockSpec(memory_space=pl.ANY)
    return pl.pallas_call(
        scatter_kernel,
        out_shape=jax.ShapeDtypeStruct((ROWS, DIM), BF16),
        in_specs=[vm, hbm, vm],
        out_specs=vm,
        scratch_shapes=[
            pltpu.VMEM((NN, TP, ROWS, NC), BF16),
            pltpu.VMEM((NN, TP - 1, ROWS, NC), BF16),
            pltpu.VMEM((NN, TP - 1, ROWS, NC), BF16),
            pltpu.VMEM((2, depth, NC), BF16),
            pltpu.SemaphoreType.DMA((2,)),
            pltpu.SemaphoreType.DMA((NN, TP - 1)),
            pltpu.SemaphoreType.DMA((NN, TP - 1)),
            pltpu.SemaphoreType.DMA((NN, TP)),
        ],
        compiler_params=pltpu.CompilerParams(collective_id=cid, has_side_effects=True, vmem_limit_bytes=VMEM_LIMIT),
        name=name,
    )(lhs, w, res)


def solution(mesh):
    row_mat = P(('dp', 'cp', 'tp'), None)
    row_vec = P(('dp', 'cp', 'tp'))
    col_split = P(None, 'tp')
    row_split = P('tp', None)

    def local_layer(hidden, positions, doc_ids, attn_gain, mlp_gain, w_query, w_key, w_value, w_out, w_gate, w_up, w_down):
        q, kv, pos = qkv_proj(hidden, attn_gain, positions, w_query, w_key, w_value)
        attn_mix = attend(q, kv, pos)
        gated, residual = mid(attn_mix, hidden, mlp_gain, w_out, w_gate, w_up)
        return scatter_proj(gated, w_down, residual, 4, "down_proj")

    in_specs = (row_mat, row_vec, row_vec, P(None), P(None), col_split, col_split, col_split, row_split, col_split, col_split, row_split)
    return jax.shard_map(local_layer, mesh=mesh, in_specs=in_specs, out_specs=row_mat, check_vma=False)
```
